32 devices in a mesh: rep: 4 (over z), row: 4 (over x, core), col: 2 (over y).
Axes of the slice: x: 2, y: 2, z: 4, core: 2. Of those that a mesh axis runs over, the one named last changes fastest.
Arguments:
- grad_parts: bfloat16 [4, 16384, 6144], P('rep', ('row', 'col')), may hold values from -0.03125 to 0.03125, as said below
- statistic: float32 [6144, 6144], P('row', 'col'), may hold values from -150 to 150, as said below
Outputs:
- gram_matrix: float32 [6144, 6144], P('row', 'col')
- statistic_next: float32 [6144, 6144], P('row', 'col')
The draws below stay inside these ranges and needn't reach their ends.
Inputs may be any that keep to these rules, and one draw needn't show every extreme that they name: Every entry of grad_parts has a magnitude between 2^-10 and 2^-5. statistic is symmetric and positive definite.
All inputs are finite; a program needn't handle non-finite values.
Results may differ from the reference program's by a relative error of at most 0.008.
Values may be sent and summed in bfloat16 or wider, within the bound.
No kernel may reach another device: no remote copies, remote signals or barrier semaphores. Data moves between devices by JAX's collectives and lax.ppermute only.
A program may use at most 192 MiB of HBM per device.

```python
import math
import jax
import jax.numpy as jnp
from jax import lax

D = 6144
HID = 16384
N_REP = 4


def draw_grad_parts(key, part):
    key_sign = jax.random.fold_in(key, 41)
    key_level = jax.random.fold_in(key, 53)
    signs = jnp.where(jax.random.bernoulli(key_sign, 0.5, (N_REP, HID, D)), 1.0, -1.0).astype(jnp.float32)
    level = jax.random.uniform(key_level, (N_REP, HID, D), jnp.float32, -10.0, -5.0)
    return (signs * jnp.exp2(level)).astype(jnp.bfloat16)


def draw_statistic(key, part):
    key_factor = jax.random.fold_in(key, 11)
    key_ridge = jax.random.fold_in(key, 23)
    factor = jax.random.truncated_normal(key_factor, -3.0, 3.0, (D, D), jnp.float32) * (2.0 / math.sqrt(D))
    crossed = jnp.dot(factor.T, factor, precision=lax.Precision.HIGHEST)
    crossed = 0.5 * (crossed + crossed.T)
    ridge = jax.random.uniform(key_ridge, (D,), jnp.float32, 0.25, 1.0)
    return crossed + jnp.diag(ridge)


def setup_inputs(seed: int = 0) -> dict:
    seeds = jax.random.split(jax.random.key(seed), 3)
    grad_parts = draw_grad_parts(jax.random.fold_in(seeds[2], 71), 0)
    statistic = draw_statistic(jax.random.fold_in(seeds[2], 71), 0)
    return {"grad_parts": grad_parts, "statistic": statistic}


def reference(grad_parts, statistic):
    summed = jnp.sum(grad_parts.astype(jnp.float32), axis=0).astype(jnp.bfloat16)
    summed = lax.optimization_barrier(summed)
    summed_f32 = summed.astype(jnp.float32)
    product = jnp.dot(summed_f32.T, summed_f32, precision=lax.Precision.HIGHEST)
    gram_full = 0.5 * (product + product.T)
    statistic_next = 0.95 * statistic + 0.05 * gram_full
    return gram_full, statistic_next
```

```python
import jax
import jax.numpy as jnp
from jax import lax
from jax.experimental import pallas as pl
from jax.experimental.pallas import tpu as pltpu
from jax.sharding import PartitionSpec as P


STRIPS = 6
PER = 1
LAG = 2
GROUPS = (
    ((0, 0), (1, 0), (1, 1)),
    *(tuple((j, i) for i in range(j + 1)) for j in range(2, STRIPS - 1)),
    tuple((STRIPS - 1, i) for i in range(STRIPS // 2)),
    tuple((STRIPS - 1, i) for i in range(STRIPS // 2, STRIPS)),
)
F32 = jnp.float32
BF16 = jnp.bfloat16


def generic(grad_parts, statistic):
    own_part = grad_parts[0].astype(F32)
    summed = lax.psum_scatter(own_part.astype(BF16), "rep", scatter_dimension=0, tiled=True)
    rows_panel = lax.all_to_all(summed, "row", split_axis=1, concat_axis=0, tiled=True)
    cols_panel = lax.all_to_all(summed, "col", split_axis=1, concat_axis=0, tiled=True)
    row_count = lax.axis_size("row")
    col_count = lax.axis_size("col")
    quarter = summed.shape[0]
    left_whole = lax.all_gather(rows_panel, "col", axis=0, tiled=True)
    left_order = (
        left_whole.reshape(col_count, row_count, quarter, -1)
        .transpose(1, 0, 2, 3)
        .reshape(row_count * col_count * quarter, -1)
    )
    partial_tile = lax.dot_general(
        left_order,
        lax.all_gather(cols_panel, "row", axis=0, tiled=True),
        (((0,), (0,)), ((), ())),
        preferred_element_type=F32,
    )
    gram_tile = lax.psum(partial_tile, "rep")
    return (gram_tile, 0.95 * statistic + 0.05 * gram_tile)


def hop_add(idx, t, own, recv, strip, slot, chunk, want_send):
    rows = own.shape[0]
    cuts = 2
    block = rows // cuts
    has_recv = recv is not None
    has_strip = strip is not None
    want_sum = slot is not None

    def body(idx_ref, *refs):
        refs = list(refs)
        value = refs.pop(0)[...]
        if has_recv:
            value = (value.astype(F32) + refs.pop(0)[...].astype(F32)).astype(BF16)
        if has_strip:
            refs.pop(0)
        if want_send:
            refs.pop(0)[...] = value
        if want_sum:
            refs.pop(0)[...] = value

    flat = pl.BlockSpec((block, chunk), lambda i, idx: (i, 0))
    own_spec = pl.BlockSpec((block, chunk), lambda i, idx: (i, idx[t]))
    in_specs = [own_spec]
    operands = [own]
    if has_recv:
        in_specs.append(flat)
        operands.append(recv)
    alias = {}
    if has_strip:
        alias = {1 + len(operands): int(want_send)}
        in_specs.append(pl.BlockSpec(memory_space=pl.ANY))
        operands.append(strip)
    out_specs, out_shape = [], []
    if want_send:
        out_specs.append(flat)
        out_shape.append(jax.ShapeDtypeStruct((rows, chunk), BF16))
    if want_sum:
        out_specs.append(pl.BlockSpec((block, chunk), lambda i, idx: (i, slot)))
        out_shape.append(jax.ShapeDtypeStruct((rows, 2 * PER * chunk), BF16))
    outs = pl.pallas_call(
        body,
        grid_spec=pltpu.PrefetchScalarGridSpec(
            num_scalar_prefetch=1, grid=(cuts,), in_specs=in_specs, out_specs=out_specs
        ),
        out_shape=out_shape,
        input_output_aliases=alias,
        compiler_params=pltpu.CompilerParams(vmem_limit_bytes=46 * 1024 * 1024),
        cost_estimate=pl.CostEstimate(flops=rows * chunk, bytes_accessed=8 * rows * chunk, transcendentals=0),
        name="hop_add",
    )(idx, *operands)
    outs = list(outs)
    return (outs.pop(0) if want_send else None), (outs.pop(0) if want_sum else strip)


def multiply(tab, strips, pairs, width):
    half = width // 2
    depth = strips[0].shape[0]
    lefts = sorted({j for j, _ in pairs})
    rights = sorted({i for _, i in pairs})
    steps = 2 * len(pairs)
    first = {j: 2 * min(p for p, pair in enumerate(pairs) if pair[0] == j) for j in lefts}

    def body(tab_ref, *refs):
        left_refs = {j: (refs[2 * k], refs[2 * k + 1]) for k, j in enumerate(lefts)}
        base = 2 * len(lefts)
        right_refs = {i: (refs[base + 2 * k], refs[base + 2 * k + 1]) for k, i in enumerate(rights)}
        send, keep, turned = refs[-3:]
        n = pl.program_id(0)
        core = tab_ref[2]
        for j in lefts:

            @pl.when(n == first[j])
            def _(j=j):
                for d in range(2):
                    turned[d * half : (d + 1) * half, :] = left_refs[j][d][...].T

        for i in rights:
            mine = [p for p, pair in enumerate(pairs) if pair[1] == i]

            @pl.when((n >= 2 * mine[0]) & (n < 2 * mine[-1] + 2))
            def _(i=i):
                far = jnp.dot(turned[...], right_refs[i][0][...], preferred_element_type=F32)
                near = jnp.dot(turned[...], right_refs[i][1][...], preferred_element_type=F32)
                send[0, :, :] = far[:half].astype(BF16)
                keep[1, :, :] = near[half:]

                @pl.when(core == 0)
                def _():
                    send[1, :, :] = near[:half].astype(BF16)
                    keep[0, :, :] = far[half:]

                @pl.when(core != 0)
                def _():
                    send[1, :, :] = far[half:].astype(BF16)
                    keep[0, :, :] = near[:half]

    in_specs, operands = [], []
    for j in lefts:
        for d in range(2):
            in_specs.append(pl.BlockSpec((depth, half), lambda n, tab, d=d: (0, tab[d])))
            operands.append(strips[j])
    for i in rights:
        mine = [p for p, pair in enumerate(pairs) if pair[1] == i]
        lo, hi = 2 * mine[0], 2 * mine[-1] + 2
        for d in range(2):
            in_specs.append(
                pl.BlockSpec(
                    (depth, half),
                    lambda n, tab, d=d, lo=lo, hi=hi: (
                        0,
                        2 * d + jnp.where(n < lo, 0, jnp.where(n >= hi, 1, n % 2)),
                    ),
                )
            )
            operands.append(strips[i])
    cols = steps * half
    out = pl.BlockSpec((2, half, half), lambda n, tab: (0, 0, n))
    return pl.pallas_call(
        body,
        grid_spec=pltpu.PrefetchScalarGridSpec(
            num_scalar_prefetch=1,
            grid=(steps,),
            in_specs=in_specs,
            out_specs=[out, out],
            scratch_shapes=[pltpu.VMEM((width, depth), BF16)],
        ),
        out_shape=[
            jax.ShapeDtypeStruct((2, half, cols), BF16),
            jax.ShapeDtypeStruct((2, half, cols), F32),
        ],
        compiler_params=pltpu.CompilerParams(vmem_limit_bytes=46 * 1024 * 1024),
        cost_estimate=pl.CostEstimate(
            flops=4 * width * depth * cols, bytes_accessed=4 * depth * cols, transcendentals=0
        ),
        name="multiply",
    )(tab, *operands)


def assemble(place, own_me, own_other, mir_me, mir_other, statistic, width):
    half = width // 2
    rows, cols = statistic.shape
    here = rows // width
    n_groups = len(GROUPS)

    def own_at(g, j, i):
        start, first = GROUPS[g][0]
        final = GROUPS[g][-1][1]
        if g == 0:
            return (j <= 1) & (i <= j), jnp.where(j == 0, 0, 1 + jnp.minimum(i, 1))
        return (j == start) & (i >= first) & (i <= final), jnp.clip(i - first, 0, final - first)

    def body(place_ref, *refs):
        me = refs[:n_groups]
        other = refs[n_groups : 2 * n_groups]
        m_me = refs[2 * n_groups : 3 * n_groups]
        m_other = refs[3 * n_groups : 4 * n_groups]
        stat, gram_out, stat_out = refs[4 * n_groups :]
        core = place_ref[0]
        j = core * here + pl.program_id(0)
        i = pl.program_id(1)
        for g in range(n_groups):
            lower, _ = own_at(g, j, i)
            upper, _ = own_at(g, i, j)

            @pl.when(lower & (core == 0))
            def _(g=g):
                gram_out[:half, :] = me[g][...]
                gram_out[half:, :] = other[g][...].astype(F32)

            @pl.when(lower & (core != 0))
            def _(g=g):
                gram_out[:half, :] = other[g][...].astype(F32)
                gram_out[half:, :] = me[g][...]

            @pl.when(upper & (i > j) & (core == 0))
            def _(g=g):
                gram_out[:, :half] = m_me[g][...].astype(F32).T
                gram_out[:, half:] = m_other[g][...].astype(F32).T

            @pl.when(upper & (i > j) & (core != 0))
            def _(g=g):
                gram_out[:, :half] = m_other[g][...].astype(F32).T
                gram_out[:, half:] = m_me[g][...].astype(F32).T

        stat_out[...] = 0.95 * stat[...] + 0.05 * gram_out[...]

    def low(g):
        def index(r, c, place):
            on, at = own_at(g, place[0] * here + r, c)
            return (0, jnp.where(on, at, 0))

        return pl.BlockSpec((half, width), index)

    def up(g):
        def index(r, c, place):
            j = place[0] * here + r
            on, at = own_at(g, c, j)
            return (0, jnp.where(on & (c > j), at, 0))

        return pl.BlockSpec((half, width), index)

    tile = pl.BlockSpec((width, width), lambda r, c, place: (r, c))
    every = range(n_groups)
    return pl.pallas_call(
        body,
        grid_spec=pltpu.PrefetchScalarGridSpec(
            num_scalar_prefetch=1,
            grid=(here, cols // width),
            in_specs=2 * [low(g) for g in every] + 2 * [up(g) for g in every] + [tile],
            out_specs=[tile, tile],
        ),
        out_shape=[jax.ShapeDtypeStruct((rows, cols), F32)] * 2,
        compiler_params=pltpu.CompilerParams(vmem_limit_bytes=28 * 1024 * 1024),
        name="assemble",
    )(place, *own_me, *own_other, *mir_me, *mir_other, statistic)


def shards(grad_parts, statistic):
    return update(grad_parts, statistic)


def update(grad_parts, statistic):
    own = grad_parts[0]
    reps = lax.axis_size("rep")
    rows_n = lax.axis_size("row")
    z = lax.axis_index("rep")
    r = lax.axis_index("row")
    x = r // 2
    core = r % 2
    y = lax.axis_index("col")
    panel = own.shape[1] // 2
    chunk = panel // (STRIPS * PER)
    width = chunk * PER
    n_chunks = STRIPS * PER * 2
    last = reps - 1
    steps = n_chunks + LAG * last
    end = (z == 0) | (z == last)

    depth = jnp.where(core == 0, z, last - z)
    c = jnp.clip(jnp.arange(steps) - LAG * depth, 0, n_chunks - 1)
    side = jnp.where((c // PER) % 2 == 0, 1 - y, y)
    idx = (side * (STRIPS * PER) + (c // (2 * PER)) * PER + c % PER).astype(jnp.int32)
    tab = jnp.stack([2 * (x != y) + core, 2 * (x == y) + core, core]).astype(jnp.int32)

    swap_core = [(i, i ^ 1) for i in range(rows_n)]

    def grid_pairs(move):
        pairs = []
        for a in range(2):
            for k in range(2):
                for b in range(2):
                    a2, k2, b2 = move(a, k, b)
                    pairs.append(((2 * a + k) * 2 + b, (2 * a2 + k2) * 2 + b2))
        return pairs

    phase_1 = grid_pairs(lambda a, k, b: (a, k, 1 - b) if k else (1 - a, k, b))
    phase_2 = grid_pairs(lambda a, k, b: (1 - a, k, b) if k else (a, k, 1 - b))
    mirror = grid_pairs(lambda a, k, b: (b, k, a))
    rc = ("row", "col")

    recvs = {}
    strips_own = []
    strip = None
    for s in range(steps):
        want_send = s < n_chunks + LAG * (last - 1)
        q = s - LAG * last
        slot = q % (2 * PER) if q >= 0 else None
        if slot == 0:
            strip = None
        send, strip = hop_add(idx, s, own, recvs.get(s - LAG), strip, slot, chunk, want_send)
        if want_send:
            pairs = []
            for k in range(last):
                if 0 <= s - LAG * k < n_chunks:
                    for i in range(rows_n):
                        a, b = (k, k + 1) if i % 2 == 0 else (last - k, last - k - 1)
                        pairs.append((a * rows_n + i, b * rows_n + i))
            recvs[s] = lax.ppermute(send, ("rep", "row"), pairs)
        if slot == 2 * PER - 1:
            strips_own.append(strip)

    holder = z == jnp.where(core == 0, last, 0)
    strips = []
    own_me, own_other, mir_me, mir_other = [], [], [], []
    for pairs in GROUPS:
        while len(strips) <= pairs[-1][0]:
            mine = strips_own[len(strips)]
            other = lax.ppermute(mine, "row", swap_core)
            strips.append(jnp.where(holder, mine, other))
        away, keep = multiply(tab, strips, pairs, width)
        got = lax.ppermute(away, rc, phase_1)
        mid = (keep[0] + got[0].astype(F32)).astype(BF16)
        got_2 = lax.ppermute(mid, rc, phase_2)
        part = (keep[1] + got[1].astype(F32) + got_2.astype(F32)).astype(BF16)

        cur = part
        total = jnp.where(end, part.astype(F32), 0.0)
        for k in range(last):
            cur = lax.ppermute(cur, "rep", sorted({(k, k + 1), (last - k, last - k - 1)}))
            total = total + cur.astype(F32)
        low = total.astype(BF16)
        there = lax.ppermute(low, rc, mirror)
        owner = pairs[-1][0] // (STRIPS // 2)
        own_other.append(lax.ppermute(low, "row", [(i, i ^ 1) for i in range(rows_n) if i % 2 != owner]))
        mir_other.append(lax.ppermute(there, "row", swap_core))
        own_me.append(total)
        mir_me.append(there)

    place = core[None].astype(jnp.int32)
    return tuple(assemble(place, own_me, own_other, mir_me, mir_other, statistic, width))


def solution(mesh):
    sizes = mesh.shape
    paired = sizes["row"] == 4 and sizes["col"] == 2 and sizes["rep"] == 4
    return jax.shard_map(
        shards if paired else generic,
        mesh=mesh,
        in_specs=(P("rep", ("row", "col"), None), P("row", "col")),
        out_specs=(P("row", "col"), P("row", "col")),
        check_vma=False,
    )
```

```python
import jax
import jax.numpy as jnp
from jax import lax
from jax.experimental import pallas as pl
from jax.experimental.pallas import tpu as pltpu
from jax.sharding import PartitionSpec as P


STRIPS = 6
PER = 1
LAG = 2
GROUPS = (
    ((0, 0), (1, 0), (1, 1)),
    *(tuple((j, i) for i in range(j + 1)) for j in range(2, STRIPS - 1)),
    tuple((STRIPS - 1, i) for i in range(STRIPS // 2)),
    tuple((STRIPS - 1, i) for i in range(STRIPS // 2, STRIPS)),
)
F32 = jnp.float32
BF16 = jnp.bfloat16


def generic(grad_parts, statistic):
    own_part = grad_parts[0].astype(F32)
    summed = lax.psum_scatter(own_part.astype(BF16), "rep", scatter_dimension=0, tiled=True)
    rows_panel = lax.all_to_all(summed, "row", split_axis=1, concat_axis=0, tiled=True)
    cols_panel = lax.all_to_all(summed, "col", split_axis=1, concat_axis=0, tiled=True)
    row_count = lax.axis_size("row")
    col_count = lax.axis_size("col")
    quarter = summed.shape[0]
    left_whole = lax.all_gather(rows_panel, "col", axis=0, tiled=True)
    left_order = (
        left_whole.reshape(col_count, row_count, quarter, -1)
        .transpose(1, 0, 2, 3)
        .reshape(row_count * col_count * quarter, -1)
    )
    partial_tile = lax.dot_general(
        left_order,
        lax.all_gather(cols_panel, "row", axis=0, tiled=True),
        (((0,), (0,)), ((), ())),
        preferred_element_type=F32,
    )
    gram_tile = lax.psum(partial_tile, "rep")
    return (gram_tile, 0.95 * statistic + 0.05 * gram_tile)


def hop_add(idx, t, own, recv, strip, slot, chunk, want_send):
    rows = own.shape[0]
    cuts = 2
    block = rows // cuts
    has_recv = recv is not None
    has_strip = strip is not None
    want_sum = slot is not None

    def body(idx_ref, *refs):
        refs = list(refs)
        value = refs.pop(0)[...]
        if has_recv:
            value = (value.astype(F32) + refs.pop(0)[...].astype(F32)).astype(BF16)
        if has_strip:
            refs.pop(0)
        if want_send:
            refs.pop(0)[...] = value
        if want_sum:
            refs.pop(0)[...] = value

    flat = pl.BlockSpec((block, chunk), lambda i, idx: (i, 0))
    own_spec = pl.BlockSpec((block, chunk), lambda i, idx: (i, idx[t]))
    in_specs = [own_spec]
    operands = [own]
    if has_recv:
        in_specs.append(flat)
        operands.append(recv)
    alias = {}
    if has_strip:
        alias = {1 + len(operands): int(want_send)}
        in_specs.append(pl.BlockSpec(memory_space=pl.ANY))
        operands.append(strip)
    out_specs, out_shape = [], []
    if want_send:
        out_specs.append(flat)
        out_shape.append(jax.ShapeDtypeStruct((rows, chunk), BF16))
    if want_sum:
        out_specs.append(pl.BlockSpec((block, chunk), lambda i, idx: (i, slot)))
        out_shape.append(jax.ShapeDtypeStruct((rows, 2 * PER * chunk), BF16))
    outs = pl.pallas_call(
        body,
        grid_spec=pltpu.PrefetchScalarGridSpec(
            num_scalar_prefetch=1, grid=(cuts,), in_specs=in_specs, out_specs=out_specs
        ),
        out_shape=out_shape,
        input_output_aliases=alias,
        compiler_params=pltpu.CompilerParams(vmem_limit_bytes=46 * 1024 * 1024),
        cost_estimate=pl.CostEstimate(flops=rows * chunk, bytes_accessed=8 * rows * chunk, transcendentals=0),
        name="hop_add",
    )(idx, *operands)
    outs = list(outs)
    return (outs.pop(0) if want_send else None), (outs.pop(0) if want_sum else strip)


def multiply(tab, strips, pairs, width):
    half = width // 2
    depth = strips[0].shape[0]
    lefts = sorted({j for j, _ in pairs})
    rights = sorted({i for _, i in pairs})
    steps = 2 * len(pairs)
    first = {j: 2 * min(p for p, pair in enumerate(pairs) if pair[0] == j) for j in lefts}

    def body(tab_ref, *refs):
        left_refs = {j: (refs[2 * k], refs[2 * k + 1]) for k, j in enumerate(lefts)}
        base = 2 * len(lefts)
        right_refs = {i: (refs[base + 2 * k], refs[base + 2 * k + 1]) for k, i in enumerate(rights)}
        send, keep, turned = refs[-3:]
        n = pl.program_id(0)
        core = tab_ref[2]
        for j in lefts:

            @pl.when(n == first[j])
            def _(j=j):
                for d in range(2):
                    turned[d * half : (d + 1) * half, :] = left_refs[j][d][...].T

        for i in rights:
            mine = [p for p, pair in enumerate(pairs) if pair[1] == i]

            @pl.when((n >= 2 * mine[0]) & (n < 2 * mine[-1] + 2))
            def _(i=i):
                far = jnp.dot(turned[...], right_refs[i][0][...], preferred_element_type=F32)
                near = jnp.dot(turned[...], right_refs[i][1][...], preferred_element_type=F32)
                send[0, :, :] = far[:half].astype(BF16)
                keep[1, :, :] = near[half:]

                @pl.when(core == 0)
                def _():
                    send[1, :, :] = near[:half].astype(BF16)
                    keep[0, :, :] = far[half:]

                @pl.when(core != 0)
                def _():
                    send[1, :, :] = far[half:].astype(BF16)
                    keep[0, :, :] = near[:half]

    in_specs, operands = [], []
    for j in lefts:
        for d in range(2):
            in_specs.append(pl.BlockSpec((depth, half), lambda n, tab, d=d: (0, tab[d])))
            operands.append(strips[j])
    for i in rights:
        mine = [p for p, pair in enumerate(pairs) if pair[1] == i]
        lo, hi = 2 * mine[0], 2 * mine[-1] + 2
        for d in range(2):
            in_specs.append(
                pl.BlockSpec(
                    (depth, half),
                    lambda n, tab, d=d, lo=lo, hi=hi: (
                        0,
                        2 * d + jnp.where(n < lo, 0, jnp.where(n >= hi, 1, n % 2)),
                    ),
                )
            )
            operands.append(strips[i])
    cols = steps * half
    out = pl.BlockSpec((2, half, half), lambda n, tab: (0, 0, n))
    return pl.pallas_call(
        body,
        grid_spec=pltpu.PrefetchScalarGridSpec(
            num_scalar_prefetch=1,
            grid=(steps,),
            in_specs=in_specs,
            out_specs=[out, out],
            scratch_shapes=[pltpu.VMEM((width, depth), BF16)],
        ),
        out_shape=[
            jax.ShapeDtypeStruct((2, half, cols), BF16),
            jax.ShapeDtypeStruct((2, half, cols), F32),
        ],
        compiler_params=pltpu.CompilerParams(vmem_limit_bytes=46 * 1024 * 1024),
        cost_estimate=pl.CostEstimate(
            flops=4 * width * depth * cols, bytes_accessed=4 * depth * cols, transcendentals=0
        ),
        name="multiply",
    )(tab, *operands)


def assemble(core, groups, blocks, own_me, own_other, mir_me, mir_other, statistic, width, made):
    half = width // 2
    rows, cols = statistic.shape
    here = rows // width
    n = len(groups)
    steps = max(len(b) for b in blocks)
    tables = [
        [b[min(k, len(b) - 1)][d] for d in range(2) for k in range(steps)] for b in blocks
    ]
    place = jnp.where(core == 0, jnp.array([0] + tables[0]), jnp.array([1] + tables[1])).astype(jnp.int32)

    def at(place, k):
        return place[1 + k], place[1 + steps + k]

    def own_at(g, j, i):
        start, first = GROUPS[g][0]
        final = GROUPS[g][-1][1]
        if g == 0:
            return (j <= 1) & (i <= j), jnp.where(j == 0, 0, 1 + jnp.minimum(i, 1))
        return (j == start) & (i >= first) & (i <= final), jnp.clip(i - first, 0, final - first)

    def body(place_ref, *refs):
        me, other, m_me, m_other = (refs[k * n : (k + 1) * n] for k in range(4))
        stat = refs[4 * n]
        gram_out, stat_out = refs[-2:]
        r, i = at(place_ref, pl.program_id(0))
        core = place_ref[0]
        j = core * here + r
        for k, g in enumerate(groups):
            lower, _ = own_at(g, j, i)
            upper, _ = own_at(g, i, j)

            @pl.when(lower)
            def _(k=k):
                gram_out[pl.ds(pl.multiple_of(core * half, half), half), :] = me[k][...]
                gram_out[pl.ds(pl.multiple_of((1 - core) * half, half), half), :] = other[k][...].astype(F32)

            @pl.when(upper & (i > j) & (core == 0))
            def _(k=k):
                gram_out[:, :half] = m_me[k][...].astype(F32).T
                gram_out[:, half:] = m_other[k][...].astype(F32).T

            @pl.when(upper & (i > j) & (core != 0))
            def _(k=k):
                gram_out[:, :half] = m_other[k][...].astype(F32).T
                gram_out[:, half:] = m_me[k][...].astype(F32).T

        stat_out[...] = 0.95 * stat[...] + 0.05 * gram_out[...]

    def low(g):
        def index(k, place):
            r, c = at(place, k)
            on, where = own_at(g, place[0] * here + r, c)
            return (0, jnp.where(on, where, 0))

        return pl.BlockSpec((half, width), index)

    def up(g):
        def index(k, place):
            r, c = at(place, k)
            j = place[0] * here + r
            on, where = own_at(g, c, j)
            return (0, jnp.where(on & (c > j), where, 1) - 1 if g == 0 else jnp.where(on & (c > j), where, 0))

        return pl.BlockSpec((half, width), index)

    tile = pl.BlockSpec((width, width), lambda k, place: at(place, k))
    tables = [[table[g] for g in groups] for table in (own_me, own_other, mir_me, mir_other)]
    operands = [*tables[0], *tables[1], *tables[2], *tables[3], statistic]
    in_specs = 2 * [low(g) for g in groups] + 2 * [up(g) for g in groups] + [tile]
    alias = {}
    if made is not None:
        alias = {1 + len(operands): 0, 2 + len(operands): 1}
        in_specs += [pl.BlockSpec(memory_space=pl.ANY)] * 2
        operands += made
    return pl.pallas_call(
        body,
        grid_spec=pltpu.PrefetchScalarGridSpec(
            num_scalar_prefetch=1, grid=(steps,), in_specs=in_specs, out_specs=[tile, tile]
        ),
        out_shape=[jax.ShapeDtypeStruct((rows, cols), F32)] * 2,
        input_output_aliases=alias,
        compiler_params=pltpu.CompilerParams(vmem_limit_bytes=50 * 1024 * 1024),
        name="assemble",
    )(place, *operands)


def shards(grad_parts, statistic):
    return update(grad_parts, statistic)


def update(grad_parts, statistic):
    own = grad_parts[0]
    reps = lax.axis_size("rep")
    rows_n = lax.axis_size("row")
    z = lax.axis_index("rep")
    r = lax.axis_index("row")
    x = r // 2
    core = r % 2
    y = lax.axis_index("col")
    panel = own.shape[1] // 2
    chunk = panel // (STRIPS * PER)
    width = chunk * PER
    n_chunks = STRIPS * PER * 2
    last = reps - 1
    steps = n_chunks + LAG * last
    end = (z == 0) | (z == last)

    depth = jnp.where(core == 0, z, last - z)
    c = jnp.clip(jnp.arange(steps) - LAG * depth, 0, n_chunks - 1)
    side = jnp.where((c // PER) % 2 == 0, 1 - y, y)
    idx = (side * (STRIPS * PER) + (c // (2 * PER)) * PER + c % PER).astype(jnp.int32)
    tab = jnp.stack([2 * (x != y) + core, 2 * (x == y) + core, core]).astype(jnp.int32)

    swap_core = [(i, i ^ 1) for i in range(rows_n)]

    def grid_pairs(move):
        pairs = []
        for a in range(2):
            for k in range(2):
                for b in range(2):
                    a2, k2, b2 = move(a, k, b)
                    pairs.append(((2 * a + k) * 2 + b, (2 * a2 + k2) * 2 + b2))
        return pairs

    phase_1 = grid_pairs(lambda a, k, b: (a, k, 1 - b) if k else (1 - a, k, b))
    phase_2 = grid_pairs(lambda a, k, b: (1 - a, k, b) if k else (a, k, 1 - b))
    mirror = grid_pairs(lambda a, k, b: (b, k, a))
    rc = ("row", "col")

    recvs = {}
    strips_own = []
    strip = None
    for s in range(steps):
        want_send = s < n_chunks + LAG * (last - 1)
        q = s - LAG * last
        slot = q % (2 * PER) if q >= 0 else None
        if slot == 0:
            strip = None
        send, strip = hop_add(idx, s, own, recvs.get(s - LAG), strip, slot, chunk, want_send)
        if want_send:
            pairs = []
            for k in range(last):
                if 0 <= s - LAG * k < n_chunks:
                    for i in range(rows_n):
                        a, b = (k, k + 1) if i % 2 == 0 else (last - k, last - k - 1)
                        pairs.append((a * rows_n + i, b * rows_n + i))
            recvs[s] = lax.ppermute(send, ("rep", "row"), pairs)
        if slot == 2 * PER - 1:
            strips_own.append(strip)

    holder = z == jnp.where(core == 0, last, 0)
    strips = []
    own_me, own_other, mir_me, mir_other = [], [], [], []
    for pairs in GROUPS:
        while len(strips) <= pairs[-1][0]:
            mine = strips_own[len(strips)]
            other = lax.ppermute(mine, "row", swap_core)
            strips.append(jnp.where(holder, mine, other))
        away, keep = multiply(tab, strips, pairs, width)
        got = lax.ppermute(away, rc, phase_1)
        mid = (keep[0] + got[0].astype(F32)).astype(BF16)
        got_2 = lax.ppermute(mid, rc, phase_2)
        part = (keep[1] + got[1].astype(F32) + got_2.astype(F32)).astype(BF16)

        cur = part
        total = jnp.where(end, part.astype(F32), 0.0)
        for k in range(last):
            cur = lax.ppermute(cur, "rep", sorted({(k, k + 1), (last - k, last - k - 1)}))
            total = total + cur.astype(F32)
        low = total.astype(BF16)
        off = [k for k, (j, i) in enumerate(pairs) if j != i]
        there = lax.ppermute(low[:, off[0] * width : (off[-1] + 1) * width], rc, mirror)
        owner = pairs[-1][0] // (STRIPS // 2)
        own_other.append(lax.ppermute(low, "row", [(i, i ^ 1) for i in range(rows_n) if i % 2 != owner]))
        mir_other.append(lax.ppermute(there, "row", swap_core))
        own_me.append(total)
        mir_me.append(there)

    here = STRIPS // 2
    edge = STRIPS - 1
    every = [[(k, i) for k in range(here) for i in range(STRIPS)] for _ in range(2)]
    late = [[(k, i) for k, i in every[c] if max(c * here + k, i) == edge] for c in range(2)]
    early = [[at for at in every[c] if at not in late[c]] for c in range(2)]
    made = None
    n_early = sum(pairs[0][0] < edge for pairs in GROUPS)
    for groups, blocks in [(range(n_early), early), (range(n_early, len(GROUPS)), late)]:
        made = assemble(core, groups, blocks, own_me, own_other, mir_me, mir_other, statistic, width, made)
    return tuple(made)


def solution(mesh):
    sizes = mesh.shape
    paired = sizes["row"] == 4 and sizes["col"] == 2 and sizes["rep"] == 4
    return jax.shard_map(
        shards if paired else generic,
        mesh=mesh,
        in_specs=(P("rep", ("row", "col"), None), P("row", "col")),
        out_specs=(P("row", "col"), P("row", "col")),
        check_vma=False,
    )
```
